32 devices in a mesh: rows: 16 (over z, y, x), cols: 2 (over core).
Axes of the slice: x: 2, y: 2, z: 4, core: 2. Of those that a mesh axis runs over, the one named last changes fastest.
Arguments:
- eigvecs: float32 [4096, 2048], P('rows', 'cols'), may hold values from -6 to 6
- reflectors: float32 [32, 4096], P('cols', 'rows'), may hold values from -17 to 17
- starts: int32 [32], replicated, may hold values from 0 to 63
Outputs:
- rotated: float32 [4096, 2048], P('rows', 'cols')
The draws below stay inside these ranges and needn't reach their ends.
Inputs may be any that keep to these rules, and one draw needn't show every extreme that they name: Sweep j's windows begin at rows starts[j] + k * 64.
All inputs are finite; a program needn't handle non-finite values.
Results may differ from the reference program's by a relative error of at most 0.00011.
Values sent between devices are 32-bit elements; how exact they have to be, the bound alone decides.
A program may use at most 64 MiB of HBM per device.

```python
import math
import jax
import jax.numpy as jnp
from jax import lax

BAND = 64
COLS = 2048
SWEEPS = 32
ORDER = 4096


def draw_reflectors(key, part):
    scale_key = jax.random.fold_in(key, 11)
    value_key = jax.random.fold_in(key, 12)
    extent = (SWEEPS, ORDER)
    scales = jnp.exp(jax.random.uniform(scale_key, extent, jnp.float32, math.log(0.3), math.log(3.0)))
    random_part = jnp.clip(jax.random.normal(value_key, extent, jnp.float32), -4.0, 4.0)
    return (random_part * scales).astype(jnp.float32)


def place_ends(values, key, low, high):
    longest = values.shape.index(max(values.shape))
    spots = []
    for shift in (0, 1):
        where = [jax.random.randint(jax.random.fold_in(key, axis), (), 0, length) for axis, length in enumerate(values.shape)]
        where[longest] = (where[longest] + shift) % values.shape[longest]
        spots.append(tuple(where))
    return values.at[spots[0]].set(low).at[spots[1]].set(high)


def levels(key, shape, cuts, smallest, high):
    loudness, own = 1.0, jax.random.fold_in(key, 6)
    for dim, parts in cuts:
        draws = jnp.exp(jax.random.uniform(jax.random.fold_in(own, dim), (parts,), jnp.float32, smallest / len(cuts), high / len(cuts)))
        loudness = loudness * jnp.repeat(draws, shape[dim] // parts).reshape([-1 if axis == dim else 1 for axis in range(len(shape))])
    return loudness


def centred(stream_key, dims, scale, limit, pieces=(), kind=jnp.bfloat16):
    result = scale * jax.random.normal(stream_key, dims, jnp.float32)
    if pieces:
        result = result * levels(stream_key, dims, pieces, -0.22, 0.18)
    return jnp.clip(result, -limit, limit).astype(kind)


def setup_inputs(seed: int = 0) -> dict:
    keys = jax.random.split(jax.random.key(seed), 4)
    eigvecs = centred(keys[0], (ORDER, COLS), 1.0, 6.0, ((0, 16), (1, 2)), jnp.float32)
    reflectors = draw_reflectors(jax.random.fold_in(keys[3], 71), 0)
    starts = place_ends(jax.random.randint(keys[2], (SWEEPS,), 0, BAND), jax.random.fold_in(keys[2], 1), 0, BAND - 1).astype(jnp.int32)
    return {"eigvecs": eigvecs, "reflectors": reflectors, "starts": starts}


def one_sweep(vectors, reflector, offset):
    total_rows = vectors.shape[0]
    blocks = total_rows // BAND
    rolled = jnp.roll(vectors, -offset, axis=0).reshape(blocks, BAND, vectors.shape[1])
    rolled_v = jnp.roll(reflector, -offset).reshape(blocks, BAND)
    squares = jnp.sum(rolled_v * rolled_v, axis=1)
    window = jnp.arange(blocks, dtype=jnp.int32)
    usable = (window + 1) * BAND + offset <= total_rows
    scaled = jnp.where(usable, 2.0 / jnp.where(usable, squares, 1.0), 0.0)
    products = jnp.einsum("kb,kbm->km", rolled_v, rolled, precision=lax.Precision.HIGHEST)
    rolled = rolled - rolled_v[:, :, None] * (scaled[:, None] * products)[:, None, :]
    return jnp.roll(rolled.reshape(total_rows, vectors.shape[1]), offset, axis=0)


def reference(eigvecs, reflectors, starts):
    def advance(sweep_idx, vectors):
        return one_sweep(vectors, reflectors[sweep_idx], starts[sweep_idx])
    return lax.fori_loop(0, SWEEPS, advance, eigvecs)
```

```python
import functools
import jax
import jax.numpy as jnp
from jax import lax
from jax.experimental import pallas as pl
from jax.experimental.pallas import tpu as pltpu
from jax.sharding import PartitionSpec as P

BAND = 64
MESH = pl.DeviceIdType.MESH
HIGH = lax.Precision.HIGHEST


def dot(a, b, ca=1, cb=0):
    return lax.dot_general(
        a, b, (((ca,), (cb,)), ((), ())), precision=HIGH, preferred_element_type=jnp.float32
    )


def sweep_ids(shape, axis, sweeps):
    return lax.broadcasted_iota(jnp.int32, shape, axis) % sweeps


def lower(gram, sweeps):
    return jnp.where(sweep_ids(gram.shape, 0, sweeps) > sweep_ids(gram.shape, 1, sweeps), gram, 0.0)


def on_diagonal(shape):
    return lax.broadcasted_iota(jnp.int32, shape, 0) == lax.broadcasted_iota(jnp.int32, shape, 1)


def inverse(full, sweeps, span):
    eye = on_diagonal(full.shape)
    diag = jnp.where(eye, full, 0.0)
    down = jnp.sum(diag, axis=1, keepdims=True)
    across = jnp.sum(diag, axis=0, keepdims=True)
    down = 1.0 / jnp.where(down == 0.0, 1.0, down)
    across = 1.0 / jnp.where(across == 0.0, 1.0, across)
    rows = sweep_ids(full.shape, 0, sweeps)
    cols = sweep_ids(full.shape, 1, sweeps)
    done = jnp.where(eye, down, 0.0)
    size = 1
    while size < span:
        part = (rows // (2 * size) == cols // (2 * size)) & (rows // size > cols // size)
        off = jnp.where(part, full, 0.0)
        if size == 1:
            done = done - down * off * across
        else:
            done = done - dot(done, dot(off, done))
        size *= 2
    return done


def kernel(nrows, ncols, x_hbm, v_ref, starts_ref, out_ref, x_ref, v_all, lt_ref, lt_in, q_send,
           q_near, q_far, p_ref, y_ref, rhs_ref, x_sem, v_local, v_send, v_recv, l_send, l_recv,
           q_send_sem, q_recv_sem):
    d, c = lax.axis_index("rows"), lax.axis_index("cols")
    own = v_ref.shape[0]
    sweeps = v_all.shape[0]
    height, width = x_ref.shape
    depth = height // BAND
    group = 2 * depth
    rounds = sweeps // group
    load = pltpu.make_async_copy(x_hbm, x_ref, x_sem)
    load.start()

    offsets = (-2, -1, 1, 2)

    def there(offset):
        return d + offset >= 0 if offset < 0 else d + offset < nrows

    barrier = pltpu.get_barrier_semaphore()
    for offset in offsets:
        @pl.when(there(offset))
        def _():
            pl.semaphore_signal(barrier, inc=1, device_id=(d + offset, c), device_id_type=MESH)
    for step in range(1, ncols):
        pl.semaphore_signal(barrier, inc=1, device_id=(d, (c + step) % ncols), device_id_type=MESH)
    for i, offset in enumerate(offsets):
        @pl.when(jnp.logical_not(there(offset)))
        def _():
            lt_in[i] = jnp.zeros_like(lt_in[i])
            for r in range(rounds):
                if abs(offset) == 1:
                    q_near[(offset + 1) // 2, r] = jnp.zeros_like(q_near[0, 0])
                else:
                    q_far[(offset + 2) // 4, r] = jnp.zeros_like(q_far[0, 0])
    y_ref[...] = jnp.zeros_like(y_ref)
    rhs_ref[...] = jnp.zeros_like(rhs_ref)
    peers = sum(there(offset).astype(jnp.int32) for offset in offsets)
    pl.semaphore_wait(barrier, peers + (ncols - 1))

    place = v_all.at[pl.ds(pl.multiple_of(c * own, own), own)]
    copies = []
    for step in range(1, ncols):
        copy = pltpu.make_async_remote_copy(
            src_ref=v_ref, dst_ref=place, send_sem=v_send.at[step - 1], recv_sem=v_recv.at[step - 1],
            device_id=(d, (c + step) % ncols), device_id_type=MESH)
        copy.start()
        copies.append(copy)
    mine = pltpu.make_async_copy(v_ref, place, v_local)
    mine.start()
    mine.wait()
    for copy in copies:
        copy.wait()

    v = v_all[...]
    begin = starts_ref[...]
    row = lax.broadcasted_iota(jnp.int32, v.shape, 1)
    window = (row - begin + BAND) // BAND
    outside = ((window == 0) & (d == 0)) | ((window == depth) & (d == nrows - 1) & (begin > 0))
    v = jnp.where(outside, 0.0, v)
    parts = [jnp.where(window == k, v, 0.0) for k in range(depth + 1)]
    u_s = jnp.concatenate([parts[0], parts[depth]], axis=0)
    u_i = jnp.concatenate(parts[1:depth], axis=0)
    half_s = 0.5 * jnp.sum(u_s * u_s, axis=1, keepdims=True)
    half_i = 0.5 * jnp.sum(u_i * u_i, axis=1, keepdims=True)
    g_ii = dot(u_i, u_i, 1, 1)
    n_si = lower(dot(u_s, u_i, 1, 1), sweeps)
    n_is = lower(dot(u_i, u_s, 1, 1), sweeps)
    g_ss = dot(u_s, u_s, 1, 1)
    l_ii = jnp.where(on_diagonal(g_ii.shape), half_i, lower(g_ii, sweeps))
    n_ss = jnp.where(on_diagonal(g_ss.shape), half_s, lower(g_ss, sweeps))
    t = inverse(l_ii, sweeps, sweeps)
    f = dot(t, n_is)
    lt = n_ss - dot(n_si, f)
    lt_ref[...] = lt

    def exchange(i, offset, src, dst, send, recv):
        return pltpu.make_async_remote_copy(
            src_ref=src, dst_ref=dst, send_sem=send, recv_sem=recv,
            device_id=(d + offset, c), device_id_type=MESH)

    def lt_copy(i, offset, slot):
        return exchange(i, offset, lt_ref, lt_in.at[slot], l_send.at[i], l_recv.at[slot])

    def q_copy(i, offset, r, slot):
        if abs(offset) == 1:
            src, dst = q_send.at[r], q_near.at[slot - 1, r]
        else:
            side = 0 if offset < 0 else 1
            src, dst = q_send.at[r, pl.ds(side * group, group)], q_far.at[slot // 3, r]
        return exchange(i, offset, src, dst, q_send_sem.at[i, r], q_recv_sem.at[slot, r])

    for i, offset in enumerate(offsets):
        @pl.when(there(offset))
        def _():
            lt_copy(i, offset, 3 - i).start()

    e = dot(t, u_i)
    b = u_s - dot(n_si, e)
    load.wait()
    x = x_ref[...]
    p_ref[...] = dot(b, x)

    def near_rows(ref, r):
        return jnp.concatenate(
            [ref[pl.ds(group * r, group)], ref[pl.ds(sweeps + group * r, group)]], axis=0)

    def send_round(r):
        q = near_rows(p_ref, r)
        if r > 0:
            q = q - dot(near_rows(lt_ref, r), y_ref[...])
        q_send[r] = q
        for i, offset in enumerate(offsets):
            @pl.when(there(offset))
            def _():
                q_copy(i, offset, r, 3 - i).start()

    send_round(0)
    ct = u_s - dot(f, u_i, 0, 0)
    out_ref[...] = x - dot(u_i, dot(e, x), 0, 0)

    for i, offset in enumerate(offsets):
        @pl.when(there(offset))
        def _():
            lt_copy(i, offset, i).wait_recv()
            lt_copy(i, offset, 3 - i).wait_send()

    def placed(block, at):
        size, total = block.shape[0], 4 * sweeps
        up = (lax.broadcasted_iota(jnp.int32, (total, size), 0)
              == lax.broadcasted_iota(jnp.int32, (total, size), 1) + at)
        up = up.astype(jnp.float32)
        return dot(dot(up, block), up, 1, 1)

    shape = lt.shape
    r_of = lax.broadcasted_iota(jnp.int32, shape, 0) // sweeps
    c_of = lax.broadcasted_iota(jnp.int32, shape, 1) // sweeps
    big = placed(lt_in[1], 0) + placed(lt, sweeps) + placed(lt_in[2], 2 * sweeps)
    big = big + placed(jnp.where((r_of == 1) & (c_of == 1), lt_in[0], 0.0), -sweeps)
    big = big + placed(jnp.where((r_of == 0) & (c_of == 0), lt_in[3], 0.0), 3 * sweeps)
    s = inverse(big, sweeps, group)

    for r in range(rounds):
        for i, offset in enumerate(offsets):
            @pl.when(there(offset))
            def _():
                q_copy(i, offset, r, i).wait_recv()
        at = group * r
        rhs_ref[pl.ds(at, group)] = q_far[0, r] + q_near[0, r, pl.ds(0, group)]
        rhs_ref[pl.ds(sweeps + at, group)] = (
            q_near[0, r, pl.ds(group, group)] + q_send[r, pl.ds(0, group)])
        rhs_ref[pl.ds(2 * sweeps + at, group)] = (
            q_send[r, pl.ds(group, group)] + q_near[1, r, pl.ds(0, group)])
        rhs_ref[pl.ds(3 * sweeps + at, group)] = q_near[1, r, pl.ds(group, group)] + q_far[1, r]
        pick = jnp.concatenate(
            [s[sweeps + at:sweeps + at + group], s[2 * sweeps + at:2 * sweeps + at + group]], axis=0)
        y = dot(pick, rhs_ref[...])
        y_ref[pl.ds(at, group)] = y[:group]
        y_ref[pl.ds(sweeps + at, group)] = y[group:]
        if r + 1 < rounds:
            send_round(r + 1)

    out_ref[...] = out_ref[...] - dot(ct, y_ref[...], 0, 0)
    for r in range(rounds):
        for i, offset in enumerate(offsets):
            @pl.when(there(offset))
            def _():
                q_copy(i, offset, r, 3 - i).wait_send()


def per_device(nrows, ncols, eigvecs, reflectors, starts):
    own, height = reflectors.shape
    width = eigvecs.shape[1]
    sweeps = starts.shape[0]
    group = 2 * (height // BAND)
    rounds = sweeps // group
    f32 = jnp.float32
    return pl.pallas_call(
        functools.partial(kernel, nrows, ncols),
        out_shape=jax.ShapeDtypeStruct((height, width), f32),
        in_specs=[pl.BlockSpec(memory_space=pl.ANY), pl.BlockSpec(memory_space=pltpu.VMEM),
                  pl.BlockSpec(memory_space=pltpu.VMEM)],
        out_specs=pl.BlockSpec(memory_space=pltpu.VMEM),
        scratch_shapes=[
            pltpu.VMEM((height, width), f32),
            pltpu.VMEM((sweeps, height), f32),
            pltpu.VMEM((2 * sweeps, 2 * sweeps), f32),
            pltpu.VMEM((4, 2 * sweeps, 2 * sweeps), f32),
            pltpu.VMEM((rounds, 2 * group, width), f32),
            pltpu.VMEM((2, rounds, 2 * group, width), f32),
            pltpu.VMEM((2, rounds, group, width), f32),
            pltpu.VMEM((2 * sweeps, width), f32),
            pltpu.VMEM((2 * sweeps, width), f32),
            pltpu.VMEM((4 * sweeps, width), f32),
            pltpu.SemaphoreType.DMA,
            pltpu.SemaphoreType.DMA,
            pltpu.SemaphoreType.DMA((ncols - 1,)),
            pltpu.SemaphoreType.DMA((ncols - 1,)),
            pltpu.SemaphoreType.DMA((4,)),
            pltpu.SemaphoreType.DMA((4,)),
            pltpu.SemaphoreType.DMA((4, rounds)),
            pltpu.SemaphoreType.DMA((4, rounds)),
        ],
        compiler_params=pltpu.CompilerParams(collective_id=0, has_side_effects=True),
    )(eigvecs, reflectors, starts.reshape(sweeps, 1))


def solution(mesh):
    in_specs = (P("rows", "cols"), P("cols", "rows"), P())
    out_specs = P("rows", "cols")
    body = functools.partial(per_device, mesh.shape["rows"], mesh.shape["cols"])
    return jax.shard_map(
        body, mesh=mesh, in_specs=in_specs, out_specs=out_specs, check_vma=False
    )
```

```python
import functools
import jax
import jax.numpy as jnp
from jax import lax
from jax.experimental import pallas as pl
from jax.experimental.pallas import tpu as pltpu
from jax.sharding import PartitionSpec as P

BAND = 64
VMEM_BYTES = 24 * 1024 * 1024
MESH = pl.DeviceIdType.MESH
HIGH = lax.Precision.HIGHEST


def dot(a, b, ca=1, cb=0):
    return lax.dot_general(
        a, b, (((ca,), (cb,)), ((), ())), precision=HIGH, preferred_element_type=jnp.float32
    )


def sweep_ids(shape, axis, sweeps):
    return lax.broadcasted_iota(jnp.int32, shape, axis) % sweeps


def lower(gram, sweeps):
    return jnp.where(sweep_ids(gram.shape, 0, sweeps) > sweep_ids(gram.shape, 1, sweeps), gram, 0.0)


def on_diagonal(shape):
    return lax.broadcasted_iota(jnp.int32, shape, 0) == lax.broadcasted_iota(jnp.int32, shape, 1)


def inverse(full, sweeps, span):
    eye = on_diagonal(full.shape)
    diag = jnp.where(eye, full, 0.0)
    down = jnp.sum(diag, axis=1, keepdims=True)
    across = jnp.sum(diag, axis=0, keepdims=True)
    down = 1.0 / jnp.where(down == 0.0, 1.0, down)
    across = 1.0 / jnp.where(across == 0.0, 1.0, across)
    rows = sweep_ids(full.shape, 0, sweeps)
    cols = sweep_ids(full.shape, 1, sweeps)
    done = jnp.where(eye, down, 0.0)
    size = 1
    while size < span:
        part = (rows // (2 * size) == cols // (2 * size)) & (rows // size > cols // size)
        off = jnp.where(part, full, 0.0)
        if size == 1:
            done = done - down * off * across
        else:
            done = done - dot(done, dot(off, done))
        size *= 2
    return done


def kernel(nrows, ncols, x_hbm, v_hbm, starts_hbm, ax_ref, ct_ref, y_ref, x_ref, v_all, starts_ref,
           lt_ref, lt_in, q_own, q_send, q_near, q_far, p_ref, x_sem, s_sem, v_local, v_send, v_recv,
           l_send, l_recv, q_send_sem, q_recv_sem):
    d, c = lax.axis_index("rows"), lax.axis_index("cols")
    own = v_hbm.shape[0]
    sweeps = v_all.shape[0]
    height, width = x_ref.shape
    depth = height // BAND
    group = 2 * depth
    rounds = sweeps // group
    place = v_all.at[pl.ds(pl.multiple_of(c * own, own), own)]
    mine = pltpu.make_async_copy(v_hbm, place, v_local)
    mine.start()
    begins = pltpu.make_async_copy(starts_hbm, starts_ref, s_sem)
    begins.start()
    load = pltpu.make_async_copy(x_hbm, x_ref, x_sem)
    load.start()

    offsets = (-2, -1, 1, 2)

    def there(offset):
        return d + offset >= 0 if offset < 0 else d + offset < nrows

    barrier = pltpu.get_barrier_semaphore()
    for offset in offsets:
        @pl.when(there(offset))
        def _():
            pl.semaphore_signal(barrier, inc=1, device_id=(d + offset, c), device_id_type=MESH)
    for step in range(1, ncols):
        pl.semaphore_signal(barrier, inc=1, device_id=(d, (c + step) % ncols), device_id_type=MESH)
    for i, offset in enumerate(offsets):
        @pl.when(jnp.logical_not(there(offset)))
        def _():
            lt_in[i] = jnp.zeros_like(lt_in[i])
            if abs(offset) == 1:
                q_near[i - 1] = jnp.zeros_like(q_near[0])
            else:
                q_far[i // 3] = jnp.zeros_like(q_far[0])
    y_ref[...] = jnp.zeros_like(y_ref)
    peers = sum(there(offset).astype(jnp.int32) for offset in offsets)
    pl.semaphore_wait(barrier, peers + (ncols - 1))

    mine.wait()
    copies = []
    for step in range(1, ncols):
        copy = pltpu.make_async_remote_copy(
            src_ref=place, dst_ref=place, send_sem=v_send.at[step - 1], recv_sem=v_recv.at[step - 1],
            device_id=(d, (c + step) % ncols), device_id_type=MESH)
        copy.start()
        copies.append(copy)
    begins.wait()
    across = jnp.broadcast_to(starts_ref[...], (sweeps, sweeps))
    begin = jnp.sum(jnp.where(on_diagonal(across.shape), across, 0), axis=1, keepdims=True)
    for copy in copies:
        copy.wait()
    v = v_all[...]
    row = lax.broadcasted_iota(jnp.int32, v.shape, 1)
    window = (row - begin + BAND) // BAND
    outside = ((window == 0) & (d == 0)) | ((window == depth) & (d == nrows - 1) & (begin > 0))
    v = jnp.where(outside, 0.0, v)
    parts = [jnp.where(window == k, v, 0.0) for k in range(depth + 1)]
    u_s = jnp.concatenate([parts[0], parts[depth]], axis=0)
    u_i = jnp.concatenate(parts[1:depth], axis=0)
    half_s = 0.5 * jnp.sum(u_s * u_s, axis=1, keepdims=True)
    half_i = 0.5 * jnp.sum(u_i * u_i, axis=1, keepdims=True)
    g_ii = dot(u_i, u_i, 1, 1)
    n_si = lower(dot(u_s, u_i, 1, 1), sweeps)
    n_is = lower(dot(u_i, u_s, 1, 1), sweeps)
    g_ss = dot(u_s, u_s, 1, 1)
    l_ii = jnp.where(on_diagonal(g_ii.shape), half_i, lower(g_ii, sweeps))
    n_ss = jnp.where(on_diagonal(g_ss.shape), half_s, lower(g_ss, sweeps))
    t = inverse(l_ii, sweeps, sweeps)
    f = dot(t, n_is)
    lt = n_ss - dot(n_si, f)
    lt_ref[...] = lt

    def exchange(i, offset, src, dst, send, recv):
        return pltpu.make_async_remote_copy(
            src_ref=src, dst_ref=dst, send_sem=send, recv_sem=recv,
            device_id=(d + offset, c), device_id_type=MESH)

    def lt_copy(i, offset, slot):
        return exchange(i, offset, lt_ref, lt_in.at[slot], l_send.at[i], l_recv.at[slot])

    def q_copy(i, offset, r, slot):
        side = 0 if offset < 0 else 1
        if abs(offset) == 1:
            src, dst = q_send.at[side, r], q_near.at[slot - 1, r]
        else:
            src, dst = q_send.at[side, r, 0], q_far.at[slot // 3, r]
        return exchange(i, offset, src, dst, q_send_sem.at[i, r], q_recv_sem.at[slot, r])

    for i, offset in enumerate(offsets):
        @pl.when(there(offset))
        def _():
            lt_copy(i, offset, 3 - i).start()

    e = dot(t, u_i)
    b = u_s - dot(n_si, e)
    load.wait()
    x = x_ref[...]
    p_ref[...] = dot(b, x)

    def near_rows(ref, r):
        return jnp.concatenate(
            [ref[pl.ds(group * r, group)], ref[pl.ds(sweeps + group * r, group)]], axis=0)

    def send_round(r):
        q = near_rows(p_ref, r)
        if r > 0:
            q = q - dot(near_rows(lt_ref, r), y_ref[...])
        q_own[r] = q
        for side in range(2):
            for part in range(2):
                q_send[side, r, part] = q[side * group + part * depth:side * group + (part + 1) * depth]
            q_send[side, r, 2] = q[(1 - side) * group:(1 - side) * group + depth]
        for i, offset in enumerate(offsets):
            @pl.when(there(offset))
            def _():
                q_copy(i, offset, r, 3 - i).start()

    send_round(0)
    ct = u_s - dot(f, u_i, 0, 0)
    ax_ref[...] = x - dot(u_i, dot(e, x), 0, 0)
    ct_ref[...] = ct

    for i, offset in enumerate(offsets):
        @pl.when(there(offset))
        def _():
            lt_copy(i, offset, i).wait_recv()
            lt_copy(i, offset, 3 - i).wait_send()

    def placed(block, at):
        size, total = block.shape[0], 4 * sweeps
        up = (lax.broadcasted_iota(jnp.int32, (total, size), 0)
              == lax.broadcasted_iota(jnp.int32, (total, size), 1) + at)
        up = up.astype(jnp.float32)
        return dot(dot(up, block), up, 1, 1)

    shape = lt.shape
    r_of = lax.broadcasted_iota(jnp.int32, shape, 0) // sweeps
    c_of = lax.broadcasted_iota(jnp.int32, shape, 1) // sweeps
    big = placed(lt_in[1], 0) + placed(lt, sweeps) + placed(lt_in[2], 2 * sweeps)
    big = big + placed(jnp.where((r_of == 1) & (c_of == 1), lt_in[0], 0.0), -sweeps)
    big = big + placed(jnp.where((r_of == 0) & (c_of == 0), lt_in[3], 0.0), 3 * sweeps)
    s = inverse(big, sweeps, group)

    compact = []
    for r in range(rounds):
        at = group * r
        pick = jnp.concatenate(
            [s[sweeps + at:sweeps + at + group], s[2 * sweeps + at:2 * sweeps + at + group]], axis=0)
        from_col = lax.broadcasted_iota(jnp.int32, (4 * sweeps, 4 * group), 0)
        to_col = lax.broadcasted_iota(jnp.int32, (4 * sweeps, 4 * group), 1)
        same = from_col == to_col // group * sweeps + at + to_col % group
        compact.append(dot(pick, same.astype(jnp.float32)))

    for r in range(rounds):
        for i, offset in enumerate(offsets):
            @pl.when(there(offset))
            def _():
                q_copy(i, offset, r, i).wait_recv()
        at = group * r
        zero = jnp.zeros((depth, width), jnp.float32)
        rhs = jnp.concatenate([
            q_far[0, r] + q_near[0, r, 2],
            zero,
            q_near[0, r, 0] + q_own[r, pl.ds(0, depth)],
            q_near[0, r, 1] + q_own[r, pl.ds(depth, depth)],
            q_near[1, r, 0] + q_own[r, pl.ds(group, depth)],
            q_near[1, r, 1] + q_own[r, pl.ds(group + depth, depth)],
            q_near[1, r, 2] + q_far[1, r],
            zero,
        ], axis=0)
        y = dot(compact[r], rhs)
        y_ref[pl.ds(at, group)] = y[:group]
        y_ref[pl.ds(sweeps + at, group)] = y[group:]
        if r + 1 < rounds:
            send_round(r + 1)

    for r in range(rounds):
        for i, offset in enumerate(offsets):
            @pl.when(there(offset))
            def _():
                q_copy(i, offset, r, 3 - i).wait_send()


def finish(ax_ref, ct_ref, y_ref, out_ref):
    out_ref[...] = ax_ref[...] - dot(ct_ref[...], y_ref[...], 0, 0)


def per_device(nrows, ncols, eigvecs, reflectors, starts):
    own, height = reflectors.shape
    width = eigvecs.shape[1]
    sweeps = starts.shape[0]
    group = 2 * (height // BAND)
    rounds = sweeps // group
    f32 = jnp.float32
    vmem = pl.BlockSpec(memory_space=pltpu.VMEM)
    hbm = pl.BlockSpec(memory_space=pltpu.HBM)
    ax, ct, y = pl.pallas_call(
        functools.partial(kernel, nrows, ncols),
        out_shape=(jax.ShapeDtypeStruct((height, width), f32),
                   jax.ShapeDtypeStruct((2 * sweeps, height), f32),
                   jax.ShapeDtypeStruct((2 * sweeps, width), f32)),
        in_specs=[hbm, hbm, hbm],
        out_specs=(vmem, vmem, vmem),
        scratch_shapes=[
            pltpu.VMEM((height, width), f32),
            pltpu.VMEM((sweeps, height), f32),
            pltpu.VMEM((1, sweeps), jnp.int32),
            pltpu.VMEM((2 * sweeps, 2 * sweeps), f32),
            pltpu.VMEM((4, 2 * sweeps, 2 * sweeps), f32),
            pltpu.VMEM((rounds, 2 * group, width), f32),
            pltpu.VMEM((2, rounds, 3, group // 2, width), f32),
            pltpu.VMEM((2, rounds, 3, group // 2, width), f32),
            pltpu.VMEM((2, rounds, group // 2, width), f32),
            pltpu.VMEM((2 * sweeps, width), f32),
            pltpu.SemaphoreType.DMA,
            pltpu.SemaphoreType.DMA,
            pltpu.SemaphoreType.DMA,
            pltpu.SemaphoreType.DMA((ncols - 1,)),
            pltpu.SemaphoreType.DMA((ncols - 1,)),
            pltpu.SemaphoreType.DMA((4,)),
            pltpu.SemaphoreType.DMA((4,)),
            pltpu.SemaphoreType.DMA((4, rounds)),
            pltpu.SemaphoreType.DMA((4, rounds)),
        ],
        compiler_params=pltpu.CompilerParams(
            collective_id=0, has_side_effects=True, vmem_limit_bytes=VMEM_BYTES),
    )(eigvecs, reflectors, starts.reshape(1, sweeps))
    tile = width // 4
    return pl.pallas_call(
        finish,
        grid=(width // tile,),
        out_shape=jax.ShapeDtypeStruct((height, width), f32),
        in_specs=[pl.BlockSpec((height, tile), lambda i: (0, i)),
                  pl.BlockSpec((2 * sweeps, height), lambda i: (0, 0)),
                  pl.BlockSpec((2 * sweeps, tile), lambda i: (0, i))],
        out_specs=pl.BlockSpec((height, tile), lambda i: (0, i)),
        compiler_params=pltpu.CompilerParams(vmem_limit_bytes=VMEM_BYTES),
    )(ax, ct, y)


def solution(mesh):
    in_specs = (P("rows", "cols"), P("cols", "rows"), P())
    out_specs = P("rows", "cols")
    body = functools.partial(per_device, mesh.shape["rows"], mesh.shape["cols"])
    return jax.shard_map(
        body, mesh=mesh, in_specs=in_specs, out_specs=out_specs, check_vma=False
    )
```

```python
import functools
import jax
import jax.numpy as jnp
from jax import lax
from jax.experimental import pallas as pl
from jax.experimental.pallas import tpu as pltpu
from jax.sharding import PartitionSpec as P

BAND = 64
MESH = pl.DeviceIdType.MESH
HIGH = lax.Precision.HIGHEST


def dot(a, b, ca=1, cb=0):
    return lax.dot_general(
        a, b, (((ca,), (cb,)), ((), ())), precision=HIGH, preferred_element_type=jnp.float32
    )


def halves(a):
    high = a.astype(jnp.bfloat16)
    return high, (a - high.astype(jnp.float32)).astype(jnp.bfloat16)


def dot_split(a, b, ca=1, cb=0):
    def one(left, right):
        return lax.dot_general(
            left, right, (((ca,), (cb,)), ((), ())), preferred_element_type=jnp.float32)
    return one(a[0], b[0]) + (one(a[0], b[1]) + one(a[1], b[0]))


def sweep_ids(shape, axis, sweeps):
    return lax.broadcasted_iota(jnp.int32, shape, axis) % sweeps


def lower(gram, sweeps):
    return jnp.where(sweep_ids(gram.shape, 0, sweeps) > sweep_ids(gram.shape, 1, sweeps), gram, 0.0)


def on_diagonal(shape):
    return lax.broadcasted_iota(jnp.int32, shape, 0) == lax.broadcasted_iota(jnp.int32, shape, 1)


def inverse(full, sweeps, span):
    eye = on_diagonal(full.shape)
    diag = jnp.where(eye, full, 0.0)
    down = jnp.sum(diag, axis=1, keepdims=True)
    across = jnp.sum(diag, axis=0, keepdims=True)
    down = 1.0 / jnp.where(down == 0.0, 1.0, down)
    across = 1.0 / jnp.where(across == 0.0, 1.0, across)
    rows = sweep_ids(full.shape, 0, sweeps)
    cols = sweep_ids(full.shape, 1, sweeps)
    done = jnp.where(eye, down, 0.0)
    size = 1
    while size < span:
        part = (rows // (2 * size) == cols // (2 * size)) & (rows // size > cols // size)
        off = jnp.where(part, full, 0.0)
        if size == 1:
            done = done - down * off * across
        else:
            done = done - dot(done, dot(off, done))
        size *= 2
    return done


def kernel(nrows, ncols, x_hbm, v_hbm, starts_hbm, ax_hbm, cm_hbm, y_hbm, x_ref, v_all, starts_ref,
           lt_ref, lt_in, q_own, q_send, q_near, q_far, p_ref, x_sem, s_sem, v_local, v_send, v_recv,
           l_send, l_recv, q_send_sem, q_recv_sem, ax_ref, cm_ref, y_ref, out_sem, y_sem):
    d, c = lax.axis_index("rows"), lax.axis_index("cols")
    own = v_hbm.shape[0]
    sweeps = v_all.shape[0]
    height, width = x_ref.shape
    depth = height // BAND
    group = 2 * depth
    rounds = sweeps // group
    place = v_all.at[pl.ds(pl.multiple_of(c * own, own), own)]
    mine = pltpu.make_async_copy(v_hbm, place, v_local)
    mine.start()
    begins = pltpu.make_async_copy(starts_hbm, starts_ref, s_sem)
    begins.start()
    load = pltpu.make_async_copy(x_hbm, x_ref, x_sem)
    load.start()

    offsets = (-2, -1, 1, 2)

    def there(offset):
        return d + offset >= 0 if offset < 0 else d + offset < nrows

    barrier = pltpu.get_barrier_semaphore()
    for offset in offsets:
        @pl.when(there(offset))
        def _():
            pl.semaphore_signal(barrier, inc=1, device_id=(d + offset, c), device_id_type=MESH)
    for step in range(1, ncols):
        pl.semaphore_signal(barrier, inc=1, device_id=(d, (c + step) % ncols), device_id_type=MESH)
    for i, offset in enumerate(offsets):
        @pl.when(jnp.logical_not(there(offset)))
        def _():
            lt_in[i] = jnp.zeros_like(lt_in[i])
            if abs(offset) == 1:
                q_near[i - 1] = jnp.zeros_like(q_near[0])
            else:
                q_far[i // 3] = jnp.zeros_like(q_far[0])
    y_ref[...] = jnp.zeros_like(y_ref)
    peers = sum(there(offset).astype(jnp.int32) for offset in offsets)
    pl.semaphore_wait(barrier, peers + (ncols - 1))

    mine.wait()
    copies = []
    for step in range(1, ncols):
        copy = pltpu.make_async_remote_copy(
            src_ref=place, dst_ref=place, send_sem=v_send.at[step - 1], recv_sem=v_recv.at[step - 1],
            device_id=(d, (c + step) % ncols), device_id_type=MESH)
        copy.start()
        copies.append(copy)
    begins.wait()
    across = jnp.broadcast_to(starts_ref[...], (sweeps, sweeps))
    begin = jnp.sum(jnp.where(on_diagonal(across.shape), across, 0), axis=1, keepdims=True)
    for copy in copies:
        copy.wait()
    v = v_all[...]
    row = lax.broadcasted_iota(jnp.int32, v.shape, 1)
    window = (row - begin + BAND) // BAND
    outside = ((window == 0) & (d == 0)) | ((window == depth) & (d == nrows - 1) & (begin > 0))
    v = jnp.where(outside, 0.0, v)
    parts = [jnp.where(window == k, v, 0.0) for k in range(depth + 1)]
    u_s = jnp.concatenate([parts[0], parts[depth]], axis=0)
    u_i = jnp.concatenate(parts[1:depth], axis=0)
    half_s = 0.5 * jnp.sum(u_s * u_s, axis=1, keepdims=True)
    half_i = 0.5 * jnp.sum(u_i * u_i, axis=1, keepdims=True)
    g_ii = dot(u_i, u_i, 1, 1)
    n_si = lower(dot(u_s, u_i, 1, 1), sweeps)
    n_is = lower(dot(u_i, u_s, 1, 1), sweeps)
    g_ss = dot(u_s, u_s, 1, 1)
    l_ii = jnp.where(on_diagonal(g_ii.shape), half_i, lower(g_ii, sweeps))
    n_ss = jnp.where(on_diagonal(g_ss.shape), half_s, lower(g_ss, sweeps))
    t = inverse(l_ii, sweeps, sweeps)
    f = dot(t, n_is)
    lt = n_ss - dot(n_si, f)
    lt_ref[...] = lt

    def exchange(i, offset, src, dst, send, recv):
        return pltpu.make_async_remote_copy(
            src_ref=src, dst_ref=dst, send_sem=send, recv_sem=recv,
            device_id=(d + offset, c), device_id_type=MESH)

    def lt_copy(i, offset, slot):
        return exchange(i, offset, lt_ref, lt_in.at[slot], l_send.at[i], l_recv.at[slot])

    def q_copy(i, offset, r, slot):
        side = 0 if offset < 0 else 1
        if abs(offset) == 1:
            src, dst = q_send.at[side, r], q_near.at[slot - 1, r]
        else:
            src, dst = q_send.at[side, r, 0], q_far.at[slot // 3, r]
        return exchange(i, offset, src, dst, q_send_sem.at[i, r], q_recv_sem.at[slot, r])

    for i, offset in enumerate(offsets):
        @pl.when(there(offset))
        def _():
            lt_copy(i, offset, 3 - i).start()

    e = dot(t, u_i)
    b = u_s - dot(n_si, e)
    load.wait()
    x_halves = halves(x_ref[...])
    p_ref[...] = dot_split(halves(b), x_halves)

    def near_rows(ref, r):
        return jnp.concatenate(
            [ref[pl.ds(group * r, group)], ref[pl.ds(sweeps + group * r, group)]], axis=0)

    def send_round(r):
        q = near_rows(p_ref, r)
        if r > 0:
            q = q - dot(near_rows(lt_ref, r), y_ref[...])
        q_own[r] = q
        for side in range(2):
            for part in range(2):
                q_send[side, r, part] = q[side * group + part * depth:side * group + (part + 1) * depth]
            q_send[side, r, 2] = q[(1 - side) * group:(1 - side) * group + depth]
        for i, offset in enumerate(offsets):
            @pl.when(there(offset))
            def _():
                q_copy(i, offset, r, 3 - i).start()

    send_round(0)
    u_t = u_i.T
    cm_ref[...] = u_s.T - dot(u_t, f)
    inner = dot_split(halves(e), x_halves)
    ax_ref[...] = x_ref[...] - dot_split(halves(u_t), halves(inner))
    outs = [pltpu.make_async_copy(ax_ref, ax_hbm, out_sem.at[0]),
            pltpu.make_async_copy(cm_ref, cm_hbm, out_sem.at[1])]
    for out in outs:
        out.start()

    for i, offset in enumerate(offsets):
        @pl.when(there(offset))
        def _():
            lt_copy(i, offset, i).wait_recv()
            lt_copy(i, offset, 3 - i).wait_send()

    def placed(block, at):
        size, total = block.shape[0], 4 * sweeps
        up = (lax.broadcasted_iota(jnp.int32, (total, size), 0)
              == lax.broadcasted_iota(jnp.int32, (total, size), 1) + at)
        up = up.astype(jnp.float32)
        return dot(dot(up, block), up, 1, 1)

    shape = lt.shape
    r_of = lax.broadcasted_iota(jnp.int32, shape, 0) // sweeps
    c_of = lax.broadcasted_iota(jnp.int32, shape, 1) // sweeps
    big = placed(lt_in[1], 0) + placed(lt, sweeps) + placed(lt_in[2], 2 * sweeps)
    big = big + placed(jnp.where((r_of == 1) & (c_of == 1), lt_in[0], 0.0), -sweeps)
    big = big + placed(jnp.where((r_of == 0) & (c_of == 0), lt_in[3], 0.0), 3 * sweeps)
    s = inverse(big, sweeps, group)

    compact = []
    for r in range(rounds):
        at = group * r
        pick = jnp.concatenate(
            [s[sweeps + at:sweeps + at + group], s[2 * sweeps + at:2 * sweeps + at + group]], axis=0)
        from_col = lax.broadcasted_iota(jnp.int32, (4 * sweeps, 4 * group), 0)
        to_col = lax.broadcasted_iota(jnp.int32, (4 * sweeps, 4 * group), 1)
        same = from_col == to_col // group * sweeps + at + to_col % group
        compact.append(dot(pick, same.astype(jnp.float32)))

    for r in range(rounds):
        for i, offset in enumerate(offsets):
            @pl.when(there(offset))
            def _():
                q_copy(i, offset, r, i).wait_recv()
        at = group * r
        zero = jnp.zeros((depth, width), jnp.float32)
        rhs = jnp.concatenate([
            q_far[0, r] + q_near[0, r, 2],
            zero,
            q_near[0, r, 0] + q_own[r, pl.ds(0, depth)],
            q_near[0, r, 1] + q_own[r, pl.ds(depth, depth)],
            q_near[1, r, 0] + q_own[r, pl.ds(group, depth)],
            q_near[1, r, 1] + q_own[r, pl.ds(group + depth, depth)],
            q_near[1, r, 2] + q_far[1, r],
            zero,
        ], axis=0)
        y = dot(compact[r], rhs)
        y_ref[pl.ds(at, group)] = y[:group]
        y_ref[pl.ds(sweeps + at, group)] = y[group:]
        if r + 1 < rounds:
            send_round(r + 1)
        for side in range(2):
            rows = pl.ds(side * sweeps + at, group)
            outs.append(pltpu.make_async_copy(y_ref.at[rows], y_hbm.at[rows], y_sem.at[side, r]))
            outs[-1].start()

    for r in range(rounds):
        for i, offset in enumerate(offsets):
            @pl.when(there(offset))
            def _():
                q_copy(i, offset, r, 3 - i).wait_send()
    for out in outs:
        out.wait()


def finish(ax_ref, cm_ref, y_ref, out_ref):
    out_ref[...] = ax_ref[...] - dot_split(halves(cm_ref[...]), halves(y_ref[...]))


def per_device(nrows, ncols, eigvecs, reflectors, starts):
    own, height = reflectors.shape
    width = eigvecs.shape[1]
    sweeps = starts.shape[0]
    group = 2 * (height // BAND)
    rounds = sweeps // group
    f32 = jnp.float32
    hbm = pl.BlockSpec(memory_space=pl.ANY)
    ax, cm, y = pl.pallas_call(
        functools.partial(kernel, nrows, ncols),
        out_shape=(jax.ShapeDtypeStruct((height, width), f32),
                   jax.ShapeDtypeStruct((height, 2 * sweeps), f32),
                   jax.ShapeDtypeStruct((2 * sweeps, width), f32)),
        in_specs=[hbm, hbm, hbm],
        out_specs=(hbm, hbm, hbm),
        scratch_shapes=[
            pltpu.VMEM((height, width), f32),
            pltpu.VMEM((sweeps, height), f32),
            pltpu.VMEM((1, sweeps), jnp.int32),
            pltpu.VMEM((2 * sweeps, 2 * sweeps), f32),
            pltpu.VMEM((4, 2 * sweeps, 2 * sweeps), f32),
            pltpu.VMEM((rounds, 2 * group, width), f32),
            pltpu.VMEM((2, rounds, 3, group // 2, width), f32),
            pltpu.VMEM((2, rounds, 3, group // 2, width), f32),
            pltpu.VMEM((2, rounds, group // 2, width), f32),
            pltpu.VMEM((2 * sweeps, width), f32),
            pltpu.SemaphoreType.DMA,
            pltpu.SemaphoreType.DMA,
            pltpu.SemaphoreType.DMA,
            pltpu.SemaphoreType.DMA((ncols - 1,)),
            pltpu.SemaphoreType.DMA((ncols - 1,)),
            pltpu.SemaphoreType.DMA((4,)),
            pltpu.SemaphoreType.DMA((4,)),
            pltpu.SemaphoreType.DMA((4, rounds)),
            pltpu.SemaphoreType.DMA((4, rounds)),
            pltpu.VMEM((height, width), f32),
            pltpu.VMEM((height, 2 * sweeps), f32),
            pltpu.VMEM((2 * sweeps, width), f32),
            pltpu.SemaphoreType.DMA((2,)),
            pltpu.SemaphoreType.DMA((2, rounds)),
        ],
        compiler_params=pltpu.CompilerParams(
            collective_id=0, has_side_effects=True),
    )(eigvecs, reflectors, starts.reshape(1, sweeps))
    tile = width // 4
    return pl.pallas_call(
        finish,
        grid=(width // tile,),
        out_shape=jax.ShapeDtypeStruct((height, width), f32),
        in_specs=[pl.BlockSpec((height, tile), lambda i: (0, i)),
                  pl.BlockSpec((height, 2 * sweeps), lambda i: (0, 0)),
                  pl.BlockSpec((2 * sweeps, tile), lambda i: (0, i))],
        out_specs=pl.BlockSpec((height, tile), lambda i: (0, i)),
    )(ax, cm, y)


def solution(mesh):
    in_specs = (P("rows", "cols"), P("cols", "rows"), P())
    out_specs = P("rows", "cols")
    body = functools.partial(per_device, mesh.shape["rows"], mesh.shape["cols"])
    return jax.shard_map(
        body, mesh=mesh, in_specs=in_specs, out_specs=out_specs, check_vma=False
    )
```

```python
import functools
import jax
import jax.numpy as jnp
from jax import lax
from jax.experimental import pallas as pl
from jax.experimental.pallas import tpu as pltpu
from jax.sharding import PartitionSpec as P

BAND = 64
MESH = pl.DeviceIdType.MESH
HIGH = lax.Precision.HIGHEST


def dot(a, b, ca=1, cb=0):
    return lax.dot_general(
        a, b, (((ca,), (cb,)), ((), ())), precision=HIGH, preferred_element_type=jnp.float32
    )


def halves(a):
    high = a.astype(jnp.bfloat16)
    return high, (a - high.astype(jnp.float32)).astype(jnp.bfloat16)


def dot_split(a, b, ca=1, cb=0):
    def one(left, right):
        return lax.dot_general(
            left, right, (((ca,), (cb,)), ((), ())), preferred_element_type=jnp.float32)
    return one(a[0], b[0]) + (one(a[0], b[1]) + one(a[1], b[0]))


def sweep_ids(shape, axis, sweeps):
    return lax.broadcasted_iota(jnp.int32, shape, axis) % sweeps


def lower(gram, sweeps):
    return jnp.where(sweep_ids(gram.shape, 0, sweeps) > sweep_ids(gram.shape, 1, sweeps), gram, 0.0)


def on_diagonal(shape):
    return lax.broadcasted_iota(jnp.int32, shape, 0) == lax.broadcasted_iota(jnp.int32, shape, 1)


def inverse(full, sweeps, span):
    eye = on_diagonal(full.shape)
    diag = jnp.where(eye, full, 0.0)
    down = jnp.sum(diag, axis=1, keepdims=True)
    across = jnp.sum(diag, axis=0, keepdims=True)
    down = 1.0 / jnp.where(down == 0.0, 1.0, down)
    across = 1.0 / jnp.where(across == 0.0, 1.0, across)
    rows = sweep_ids(full.shape, 0, sweeps)
    cols = sweep_ids(full.shape, 1, sweeps)
    done = jnp.where(eye, down, 0.0)
    size = 1
    while size < span:
        part = (rows // (2 * size) == cols // (2 * size)) & (rows // size > cols // size)
        off = jnp.where(part, full, 0.0)
        if size == 1:
            done = done - down * off * across
        else:
            done = done - dot(done, dot(off, done))
        size *= 2
    return done


def kernel(nrows, ncols, x_hbm, v_hbm, starts_hbm, ax_hbm, cm_hbm, y_hbm, x_ref, v_all, starts_ref,
           lt_ref, lt_in, q_own, q_send, q_near, q_far, p_ref, x_sem, s_sem, v_local, v_send, v_recv,
           l_send, l_recv, q_send_sem, q_recv_sem, ax_ref, cm_ref, y_ref, out_sem, y_sem):
    d, c = lax.axis_index("rows"), lax.axis_index("cols")
    own = v_hbm.shape[0]
    sweeps = v_all.shape[0]
    height, width = x_ref.shape
    depth = height // BAND
    group = 2 * depth
    rounds = sweeps // group
    place = v_all.at[pl.ds(pl.multiple_of(c * own, own), own)]
    mine = pltpu.make_async_copy(v_hbm, place, v_local)
    mine.start()
    begins = pltpu.make_async_copy(starts_hbm, starts_ref, s_sem)
    begins.start()
    load = pltpu.make_async_copy(x_hbm, x_ref, x_sem)
    load.start()

    offsets = (-2, -1, 1, 2)

    def there(offset):
        return d + offset >= 0 if offset < 0 else d + offset < nrows

    barrier = pltpu.get_barrier_semaphore()
    for offset in offsets:
        @pl.when(there(offset))
        def _():
            pl.semaphore_signal(barrier, inc=1, device_id=(d + offset, c), device_id_type=MESH)
    for step in range(1, ncols):
        pl.semaphore_signal(barrier, inc=1, device_id=(d, (c + step) % ncols), device_id_type=MESH)
    for i, offset in enumerate(offsets):
        @pl.when(jnp.logical_not(there(offset)))
        def _():
            lt_in[i] = jnp.zeros_like(lt_in[i])
            if abs(offset) == 1:
                q_near[i - 1] = jnp.zeros_like(q_near[0])
            else:
                q_far[i // 3] = jnp.zeros_like(q_far[0])
    y_ref[...] = jnp.zeros_like(y_ref)
    peers = sum(there(offset).astype(jnp.int32) for offset in offsets)
    pl.semaphore_wait(barrier, peers + (ncols - 1))

    mine.wait()
    copies = []
    for step in range(1, ncols):
        copy = pltpu.make_async_remote_copy(
            src_ref=place, dst_ref=place, send_sem=v_send.at[step - 1], recv_sem=v_recv.at[step - 1],
            device_id=(d, (c + step) % ncols), device_id_type=MESH)
        copy.start()
        copies.append(copy)
    begins.wait()
    across = jnp.broadcast_to(starts_ref[...], (sweeps, sweeps))
    begin = jnp.sum(jnp.where(on_diagonal(across.shape), across, 0), axis=1, keepdims=True)
    for copy in copies:
        copy.wait()
    v = v_all[...]
    row = lax.broadcasted_iota(jnp.int32, v.shape, 1)
    window = (row - begin + BAND) // BAND
    outside = ((window == 0) & (d == 0)) | ((window == depth) & (d == nrows - 1) & (begin > 0))
    v = jnp.where(outside, 0.0, v)
    parts = [jnp.where(window == k, v, 0.0) for k in range(depth + 1)]
    u_s = jnp.concatenate([parts[0], parts[depth]], axis=0)
    u_i = jnp.concatenate(parts[1:depth], axis=0)
    half_s = 0.5 * jnp.sum(u_s * u_s, axis=1, keepdims=True)
    half_i = 0.5 * jnp.sum(u_i * u_i, axis=1, keepdims=True)
    g_ii = dot(u_i, u_i, 1, 1)
    n_si = lower(dot(u_s, u_i, 1, 1), sweeps)
    n_is = lower(dot(u_i, u_s, 1, 1), sweeps)
    g_ss = dot(u_s, u_s, 1, 1)
    l_ii = jnp.where(on_diagonal(g_ii.shape), half_i, lower(g_ii, sweeps))
    n_ss = jnp.where(on_diagonal(g_ss.shape), half_s, lower(g_ss, sweeps))
    t = inverse(l_ii, sweeps, sweeps)
    f = dot(t, n_is)
    lt = n_ss - dot(n_si, f)
    lt_ref[...] = lt

    def exchange(i, offset, src, dst, send, recv):
        return pltpu.make_async_remote_copy(
            src_ref=src, dst_ref=dst, send_sem=send, recv_sem=recv,
            device_id=(d + offset, c), device_id_type=MESH)

    def lt_copy(i, offset, slot):
        return exchange(i, offset, lt_ref, lt_in.at[slot], l_send.at[i], l_recv.at[slot])

    def q_copy(i, offset, r, slot):
        side = 0 if offset < 0 else 1
        if abs(offset) == 1:
            src, dst = q_send.at[side, r], q_near.at[slot - 1, r]
        else:
            src, dst = q_send.at[side, r, 0], q_far.at[slot // 3, r]
        return exchange(i, offset, src, dst, q_send_sem.at[i, r], q_recv_sem.at[slot, r])

    for i, offset in enumerate(offsets):
        @pl.when(there(offset))
        def _():
            lt_copy(i, offset, 3 - i).start()

    e = dot(t, u_i)
    b = u_s - dot(n_si, e)
    load.wait()
    x_halves = halves(x_ref[...])
    p_ref[...] = dot_split(halves(b), x_halves)

    def near_rows(ref, r):
        return jnp.concatenate(
            [ref[pl.ds(group * r, group)], ref[pl.ds(sweeps + group * r, group)]], axis=0)

    def send_round(r):
        q = near_rows(p_ref, r)
        if r > 0:
            q = q - dot_split(halves(near_rows(lt_ref, r)), halves(y_ref[...]))
        q_own[r] = q
        for side in range(2):
            for part in range(2):
                q_send[side, r, part] = q[side * group + part * depth:side * group + (part + 1) * depth]
            q_send[side, r, 2] = q[(1 - side) * group:(1 - side) * group + depth]
        for i, offset in enumerate(offsets):
            @pl.when(there(offset))
            def _():
                q_copy(i, offset, r, 3 - i).start()

    send_round(0)
    u_t = u_i.T
    cm_ref[...] = u_s.T - dot(u_t, f)
    inner = dot_split(halves(e), x_halves)
    ax_ref[...] = x_ref[...] - dot_split(halves(u_t), halves(inner))
    outs = [pltpu.make_async_copy(ax_ref, ax_hbm, out_sem.at[0]),
            pltpu.make_async_copy(cm_ref, cm_hbm, out_sem.at[1])]
    for out in outs:
        out.start()

    for i, offset in enumerate(offsets):
        @pl.when(there(offset))
        def _():
            lt_copy(i, offset, i).wait_recv()
            lt_copy(i, offset, 3 - i).wait_send()

    def placed(block, at):
        size, total = block.shape[0], 4 * sweeps
        up = (lax.broadcasted_iota(jnp.int32, (total, size), 0)
              == lax.broadcasted_iota(jnp.int32, (total, size), 1) + at)
        up = up.astype(jnp.float32)
        return dot(dot(up, block), up, 1, 1)

    shape = lt.shape
    r_of = lax.broadcasted_iota(jnp.int32, shape, 0) // sweeps
    c_of = lax.broadcasted_iota(jnp.int32, shape, 1) // sweeps
    big = placed(lt_in[1], 0) + placed(lt, sweeps) + placed(lt_in[2], 2 * sweeps)
    big = big + placed(jnp.where((r_of == 1) & (c_of == 1), lt_in[0], 0.0), -sweeps)
    big = big + placed(jnp.where((r_of == 0) & (c_of == 0), lt_in[3], 0.0), 3 * sweeps)
    s = inverse(big, sweeps, group)

    compact = []
    for r in range(rounds):
        at = group * r
        pick = jnp.concatenate(
            [s[sweeps + at:sweeps + at + group], s[2 * sweeps + at:2 * sweeps + at + group]], axis=0)
        from_col = lax.broadcasted_iota(jnp.int32, (4 * sweeps, 4 * group), 0)
        to_col = lax.broadcasted_iota(jnp.int32, (4 * sweeps, 4 * group), 1)
        same = from_col == to_col // group * sweeps + at + to_col % group
        compact.append(halves(dot(pick, same.astype(jnp.float32))))

    for r in range(rounds):
        for i, offset in enumerate(offsets):
            @pl.when(there(offset))
            def _():
                q_copy(i, offset, r, i).wait_recv()
        at = group * r
        zero = jnp.zeros((depth, width), jnp.float32)
        rhs = jnp.concatenate([
            q_far[0, r] + q_near[0, r, 2],
            zero,
            q_near[0, r, 0] + q_own[r, pl.ds(0, depth)],
            q_near[0, r, 1] + q_own[r, pl.ds(depth, depth)],
            q_near[1, r, 0] + q_own[r, pl.ds(group, depth)],
            q_near[1, r, 1] + q_own[r, pl.ds(group + depth, depth)],
            q_near[1, r, 2] + q_far[1, r],
            zero,
        ], axis=0)
        y = dot_split(compact[r], halves(rhs))
        y_ref[pl.ds(at, group)] = y[:group]
        y_ref[pl.ds(sweeps + at, group)] = y[group:]
        if r + 1 < rounds:
            send_round(r + 1)
        for side in range(2):
            rows = pl.ds(side * sweeps + at, group)
            outs.append(pltpu.make_async_copy(y_ref.at[rows], y_hbm.at[rows], y_sem.at[side, r]))
            outs[-1].start()

    for r in range(rounds):
        for i, offset in enumerate(offsets):
            @pl.when(there(offset))
            def _():
                q_copy(i, offset, r, 3 - i).wait_send()
    for out in outs:
        out.wait()


def finish(ax_ref, cm_ref, y_ref, out_ref):
    out_ref[...] = ax_ref[...] - dot_split(halves(cm_ref[...]), halves(y_ref[...]))


def per_device(nrows, ncols, eigvecs, reflectors, starts):
    own, height = reflectors.shape
    width = eigvecs.shape[1]
    sweeps = starts.shape[0]
    group = 2 * (height // BAND)
    rounds = sweeps // group
    f32 = jnp.float32
    hbm = pl.BlockSpec(memory_space=pl.ANY)
    ax, cm, y = pl.pallas_call(
        functools.partial(kernel, nrows, ncols),
        out_shape=(jax.ShapeDtypeStruct((height, width), f32),
                   jax.ShapeDtypeStruct((height, 2 * sweeps), f32),
                   jax.ShapeDtypeStruct((2 * sweeps, width), f32)),
        in_specs=[hbm, hbm, hbm],
        out_specs=(hbm, hbm, hbm),
        scratch_shapes=[
            pltpu.VMEM((height, width), f32),
            pltpu.VMEM((sweeps, height), f32),
            pltpu.VMEM((1, sweeps), jnp.int32),
            pltpu.VMEM((2 * sweeps, 2 * sweeps), f32),
            pltpu.VMEM((4, 2 * sweeps, 2 * sweeps), f32),
            pltpu.VMEM((rounds, 2 * group, width), f32),
            pltpu.VMEM((2, rounds, 3, group // 2, width), f32),
            pltpu.VMEM((2, rounds, 3, group // 2, width), f32),
            pltpu.VMEM((2, rounds, group // 2, width), f32),
            pltpu.VMEM((2 * sweeps, width), f32),
            pltpu.SemaphoreType.DMA,
            pltpu.SemaphoreType.DMA,
            pltpu.SemaphoreType.DMA,
            pltpu.SemaphoreType.DMA((ncols - 1,)),
            pltpu.SemaphoreType.DMA((ncols - 1,)),
            pltpu.SemaphoreType.DMA((4,)),
            pltpu.SemaphoreType.DMA((4,)),
            pltpu.SemaphoreType.DMA((4, rounds)),
            pltpu.SemaphoreType.DMA((4, rounds)),
            pltpu.VMEM((height, width), f32),
            pltpu.VMEM((height, 2 * sweeps), f32),
            pltpu.VMEM((2 * sweeps, width), f32),
            pltpu.SemaphoreType.DMA((2,)),
            pltpu.SemaphoreType.DMA((2, rounds)),
        ],
        compiler_params=pltpu.CompilerParams(
            collective_id=0, has_side_effects=True),
    )(eigvecs, reflectors, starts.reshape(1, sweeps))
    tile = width // 2
    return pl.pallas_call(
        finish,
        grid=(width // tile,),
        out_shape=jax.ShapeDtypeStruct((height, width), f32),
        in_specs=[pl.BlockSpec((height, tile), lambda i: (0, i)),
                  pl.BlockSpec((height, 2 * sweeps), lambda i: (0, 0)),
                  pl.BlockSpec((2 * sweeps, tile), lambda i: (0, i))],
        out_specs=pl.BlockSpec((height, tile), lambda i: (0, i)),
    )(ax, cm, y)


def solution(mesh):
    in_specs = (P("rows", "cols"), P("cols", "rows"), P())
    out_specs = P("rows", "cols")
    body = functools.partial(per_device, mesh.shape["rows"], mesh.shape["cols"])
    return jax.shard_map(
        body, mesh=mesh, in_specs=in_specs, out_specs=out_specs, check_vma=False
    )
```
